32 devices in a mesh: lat: 4 (over y, x), lon: 8 (over z, core).
Axes of the slice: x: 2, y: 2, z: 4, core: 2. Of those that a mesh axis runs over, the one named last changes fastest.
Arguments:
- pressure: float32 [4, 30, 5120], P('lat', None, 'lon'), may hold values from -6 to 6
- velocity: float32 [4, 30, 7680], P('lat', None, 'lon'), may hold values from -6 to 6
- edge_cells: int32 [4, 2, 7680], P('lat', None, 'lon'), may hold values from 0 to 1663
- cell_edges: int32 [4, 3, 5120], P('lat', None, 'lon'), may hold values from 0 to 1983
- send_cells: int32 [4, 8, 1024], P('lat', None, 'lon'), may hold values from 0 to 639
- send_edges: int32 [4, 8, 1024], P('lat', None, 'lon'), may hold values from 0 to 959
- inv_dual: float32 [4, 7680], P('lat', 'lon'), may hold values from 0.5 to 2
- edge_weight: float32 [4, 3, 5120], P('lat', None, 'lon'), may hold values from -3 to 3
- sound_speed: float32 [4, 5120], P('lat', 'lon'), may hold values from 0.1 to 0.6
- coupling: float32 [4, 30, 5120], P('lat', None, 'lon'), may hold values from 0.1 to 2
Outputs:
- pressure_out: float32 [4, 30, 5120], P('lat', None, 'lon')
- velocity_out: float32 [4, 30, 7680], P('lat', None, 'lon')
The draws below stay inside these ranges and needn't reach their ends.
Inputs may be any that keep to these rules, and one draw needn't show every extreme that they name: `edge_cells`: positions below 640 are own cells; position 640 + r * 128 + j is slot j of the halo piece from the neighbour at offset number r. `cell_edges`: positions below 960 are own edges; position 960 + r * 128 + j is slot j of the edge halo piece from the neighbour at offset number r. `send_cells`: indices of own cells. `send_edges`: indices of own edges.
All inputs are finite; a program needn't handle non-finite values.
Results may differ from the reference program's by a relative error of at most 0.0001.
Values sent between devices are 32-bit elements; how exact they have to be, the bound alone decides.
A program may use at most 64 MiB of HBM per device.

```python
import math
import jax
import jax.numpy as jnp
from jax import lax

C_DEV = 640
E_DEV = 960
HALO = 128
NLEV = 30
NSUB = 3
CELLS_ROW = 5120
EDGES_ROW = 7680
SLOTS_ROW = 1024
N_LAT = 4
N_LON = 8


def with_ends(values, own_key, smallest, largest):
    spot = [jax.random.randint(jax.random.fold_in(own_key, axis), (), 0, length) for axis, length in enumerate(values.shape)]
    longest = values.shape.index(max(values.shape))
    neighbour = spot[:longest] + [(spot[longest] + 1) % values.shape[longest]] + spot[longest + 1:]
    return values.at[tuple(spot)].set(smallest).at[tuple(neighbour)].set(largest)


def block_levels(own_key, dims, cuts, low, top_value):
    factor_of, own = 1.0, jax.random.fold_in(own_key, 6)
    for dim, shards_of in cuts:
        heights = jnp.exp(jax.random.uniform(jax.random.fold_in(own, dim), (shards_of,), jnp.float32, low / len(cuts), top_value / len(cuts)))
        factor_of = factor_of * jnp.repeat(heights, dims[dim] // shards_of).reshape([-1 if axis == dim else 1 for axis in range(len(dims))])
    return factor_of


def normal_values(rng, extent, scale, bound, cuts=(), kind=jnp.bfloat16):
    values = scale * jax.random.normal(rng, extent, jnp.float32)
    if cuts:
        values = values * block_levels(rng, extent, cuts, -0.22, 0.18)
    return jnp.clip(values, -bound, bound).astype(kind)


def setup_inputs(seed: int = 0) -> dict:
    streams_of = jax.random.split(jax.random.key(seed), 11)
    return {
        "pressure": normal_values(streams_of[0], (N_LAT, NLEV, CELLS_ROW), 1.0, 6.0, ((0, 4), (2, 8)), jnp.float32),
        "velocity": normal_values(streams_of[1], (N_LAT, NLEV, EDGES_ROW), 1.0, 6.0, ((0, 4), (2, 8)), jnp.float32),
        "edge_cells": with_ends(jax.random.randint(streams_of[2], (N_LAT, 2, EDGES_ROW), 0, C_DEV + 8 * HALO), jax.random.fold_in(streams_of[2], 1), 0, (C_DEV + 8 * HALO) - 1).astype(jnp.int32),
        "cell_edges": with_ends(jax.random.randint(streams_of[3], (N_LAT, 3, CELLS_ROW), 0, E_DEV + 8 * HALO), jax.random.fold_in(streams_of[3], 1), 0, (E_DEV + 8 * HALO) - 1).astype(jnp.int32),
        "send_cells": with_ends(jax.random.randint(streams_of[4], (N_LAT, 8, SLOTS_ROW), 0, C_DEV), jax.random.fold_in(streams_of[4], 1), 0, C_DEV - 1).astype(jnp.int32),
        "send_edges": with_ends(jax.random.randint(streams_of[5], (N_LAT, 8, SLOTS_ROW), 0, E_DEV), jax.random.fold_in(streams_of[5], 1), 0, E_DEV - 1).astype(jnp.int32),
        "inv_dual": jnp.clip(jnp.exp(math.log(2.0) - 1.3862944 * jax.random.uniform(streams_of[6], (N_LAT, EDGES_ROW), jnp.float32) ** block_levels(streams_of[6], (N_LAT, EDGES_ROW), ((0, 4), (1, 8)), -0.2, 0.2)), 0.5, 2.0),
        "edge_weight": normal_values(streams_of[7], (N_LAT, 3, CELLS_ROW), 0.5, 3.0, ((0, 4), (2, 8)), jnp.float32),
        "sound_speed": jnp.clip(jnp.exp(math.log(0.6) - 1.7917595 * jax.random.uniform(streams_of[8], (N_LAT, CELLS_ROW), jnp.float32) ** block_levels(streams_of[8], (N_LAT, CELLS_ROW), ((0, 4), (1, 8)), -0.2, 0.2)), 0.1, 0.6),
        "coupling": jnp.clip(jnp.exp(math.log(2.0) - 2.9957323 * jax.random.uniform(streams_of[9], (N_LAT, NLEV, CELLS_ROW), jnp.float32) ** block_levels(streams_of[9], (N_LAT, NLEV, CELLS_ROW), ((0, 4), (2, 8)), -0.2, 0.2)), 0.1, 2.0),
    }


DIRECTIONS = ((-1, -1), (-1, 0), (-1, 1), (0, -1), (0, 1), (1, -1), (1, 0), (1, 1))
step_scale = 0.5


def position(offset):
    return DIRECTIONS.index(offset)


def edge_update(normal, extended, edge_cells, inv_dual):
    gradient = (jnp.take(extended, edge_cells[1], axis=1) - jnp.take(extended, edge_cells[0], axis=1)) * inv_dual[None, :]
    return normal - step_scale * gradient


def column_solve(right_side, coupling):
    levels = right_side.shape[0]
    ratios = []
    scaled = []
    for level_index in range(levels):
        if level_index < levels - 1:
            upper_term = -coupling[level_index]
        else:
            upper_term = 0.0 * coupling[0]
        if level_index == 0:
            divisor = 1.0 + coupling[0]
            current = right_side[0] / divisor
        else:
            lower_term = -coupling[level_index - 1]
            diagonal = 1.0 + coupling[level_index - 1] + coupling[level_index]
            divisor = diagonal - lower_term * ratios[-1]
            current = (right_side[level_index] - lower_term * scaled[-1]) / divisor
        ratios.append(upper_term / divisor)
        scaled.append(current)
    result = [scaled[-1]]
    for level_index in range(levels - 2, -1, -1):
        result.insert(0, scaled[level_index] - ratios[level_index] * result[0])
    return jnp.stack(result)


def cell_update(values, edges_ext, cell_edges, edge_weight, sound_speed, coupling):
    divergence = jnp.take(edges_ext, cell_edges[0], axis=1) * edge_weight[0][None, :]
    divergence = divergence + jnp.take(edges_ext, cell_edges[1], axis=1) * edge_weight[1][None, :]
    divergence = divergence + jnp.take(edges_ext, cell_edges[2], axis=1) * edge_weight[2][None, :]
    right_side = values - sound_speed[None, :] * divergence
    return column_solve(right_side, coupling)


def device_layout(array, width):
    if array.ndim == 2:
        return array.reshape(N_LAT, N_LON, width)
    return array.reshape(N_LAT, array.shape[1], N_LON, width).transpose(0, 2, 1, 3)


def global_layout(array):
    return array.transpose(0, 2, 1, 3).reshape(N_LAT, array.shape[2], N_LON * array.shape[3])


def take_pieces(source, indices):
    return jnp.take(source, indices, axis=1)


def reference_extend(source, send_list):
    taker = jax.vmap(jax.vmap(take_pieces))
    pieces = []
    for offset in DIRECTIONS:
        piece = taker(source, send_list[:, :, position((-offset[0], -offset[1]))])
        piece = jnp.roll(piece, -offset[1], axis=1)
        if offset[0] == 1:
            piece = jnp.concatenate([piece[1:], jnp.zeros_like(piece[:1])], axis=0)
        elif offset[0] == -1:
            piece = jnp.concatenate([jnp.zeros_like(piece[:1]), piece[:-1]], axis=0)
        pieces.append(piece)
    return jnp.concatenate([source] + pieces, axis=3)


def band_edges(operands):
    return jax.vmap(edge_update)(*operands)


def band_cells(operands):
    return jax.vmap(cell_update)(*operands)


def reference(pressure, velocity, edge_cells, cell_edges, send_cells, send_edges, inv_dual, edge_weight, sound_speed, coupling):
    values = device_layout(pressure, C_DEV)
    normal = device_layout(velocity, E_DEV)
    edge_pairs = device_layout(edge_cells, E_DEV)
    cell_sides = device_layout(cell_edges, C_DEV)
    cell_lists = device_layout(send_cells, HALO)
    edge_lists = device_layout(send_edges, HALO)
    inverse = device_layout(inv_dual, E_DEV)
    weights = device_layout(edge_weight, C_DEV)
    speeds = device_layout(sound_speed, C_DEV)
    couples = device_layout(coupling, C_DEV)
    for substep in range(NSUB):
        extended = reference_extend(values, cell_lists)
        normal = lax.map(band_edges, (normal, extended, edge_pairs, inverse))
        edges_ext = reference_extend(normal, edge_lists)
        values = lax.map(band_cells, (values, edges_ext, cell_sides, weights, speeds, couples))
    return global_layout(values), global_layout(normal)
```

```python
import math

import jax
import jax.numpy as jnp
from jax import lax
from jax.experimental import pallas as pl
from jax.experimental.pallas import tpu as pltpu
from jax.sharding import PartitionSpec as P

NSUB = 3
OFFSETS = ((-1, -1), (-1, 0), (-1, 1), (0, -1), (0, 1), (1, -1), (1, 0), (1, 1))
LANES = 128
step_scale = 0.5
MESH = pl.DeviceIdType.MESH
F32 = jnp.float32


def round_up(n, m):
    return (n + m - 1) // m * m


def tiles_of(ref, width):
    return [ref[:, k * LANES : (k + 1) * LANES] for k in range(width // LANES)]


def spread(index, own, padded):
    return jnp.where(index >= own, index + (padded - own), index)


def member_of(p, q):
    if isinstance(p, int) and p == 0:
        return 3 + (q + 1) // 2
    return (7 + 5 * p) // 2 + q


def kernel(
    n_lat, n_lon, nlev, cells, edges, halo,
    p_hbm, v_hbm, ec_hbm, ce_hbm, sc_hbm, se_hbm, inv_hbm, weight_hbm, sound_hbm, coupling_hbm,
    p_out, v_out,
    p_row, v_row, ec, ce, sc, se, inv_dual, weight, sound, coupling,
    pf, vf, p_send, v_send, p_halo, v_halo,
    t_inv, t_low, t_up, t_mid, work, grad, div,
    sc_list, se_list, ec_list, ce_list, scale_list, weight_list, sound_list,
    s_inv, s_low, s_up, s_mid, s_grad, s_div,
    p_ss, p_rs, v_ss, v_rs, in_sem,
):
    a, b = lax.axis_index("lat"), lax.axis_index("lon")
    ccols, ecols = pf.shape[1], vf.shape[1]
    rows = pf.shape[0]
    pieces = len(OFFSETS)
    middle = nlev // 2
    side = math.isqrt(n_lat)
    slow = jnp.where(lax.rem(a, side) == side - 1, 1, -1)
    quick = -slow
    far = 2 * lax.rem(b, 2) - 1
    near = -far
    sends = [
        (slow, far), (slow, near), (slow, 0), (quick, far), (0, far),
        (quick, near), (quick, 0), (0, near),
    ]
    p_batches = (range(0, 1), range(1, 5), range(5, 8),)
    v_batches = (range(0, 1), range(1, 3), range(3, 5), range(5, 8),)

    def if_there(p, fn):
        if isinstance(p, int) and p == 0:
            fn()
        else:
            pl.when((a + p >= 0) & (a + p < n_lat))(fn)

    def target(p, q):
        return (a + p, lax.rem(b + q + n_lon, n_lon))

    barrier = pltpu.get_barrier_semaphore()
    for lat_step in (-1, 1, 0):
        def greet(lat_step=lat_step):
            for offset in OFFSETS:
                if offset[0] == lat_step:
                    pl.semaphore_signal(
                        barrier, inc=1, device_id=target(*offset), device_id_type=MESH
                    )
        if_there(lat_step, greet)

    pairs = [
        (p_hbm, p_row), (sc_hbm, sc), (ec_hbm, ec), (v_hbm, v_row), (se_hbm, se),
        (inv_hbm, inv_dual), (coupling_hbm, coupling), (ce_hbm, ce), (weight_hbm, weight), (sound_hbm, sound),
    ]
    loads = [pltpu.make_async_copy(x, y, in_sem.at[k]) for k, (x, y) in enumerate(pairs)]
    for load in loads:
        load.start()

    def clear(p):
        def fill():
            for slot, offset in enumerate(OFFSETS):
                if offset[0] == p:
                    for turn in range(2):
                        p_halo[turn, slot] = jnp.zeros(p_halo.shape[2:], F32)
                        v_halo[turn, slot] = jnp.zeros(v_halo.shape[2:], F32)
        return fill

    pl.when(a == 0)(clear(-1))
    pl.when(a == n_lat - 1)(clear(1))
    pf[nlev - nlev % 8 :, :] = jnp.zeros_like(pf[nlev - nlev % 8 :, :])
    work[nlev - nlev % 8 :, :] = jnp.zeros_like(pf[nlev - nlev % 8 :, :])
    vf[...] = jnp.zeros_like(vf)

    def copy(i, send, land, ss, rs, turn):
        p, q = sends[i]
        member = member_of(p, q)
        return pltpu.make_async_remote_copy(
            src_ref=send.at[pl.ds(i * rows, rows)], dst_ref=land.at[turn, 7 - member],
            send_sem=ss.at[i], recv_sem=rs.at[7 - member],
            device_id=target(p, q), device_id_type=MESH,
        )

    def launch(batch, refs, turn):
        for i in batch:
            if_there(sends[i][0], lambda: copy(i, *refs, turn).start())

    def arrive(group, refs, turn):
        send, land, ss, rs = refs
        for p, q in group:
            slot = member_of(p, q)

            def wait():
                pltpu.make_async_remote_copy(
                    src_ref=send.at[pl.ds(0, rows)], dst_ref=land.at[turn, slot],
                    send_sem=ss.at[0], recv_sem=rs.at[slot],
                    device_id=target(p, q), device_id_type=MESH,
                ).wait_recv()
            if_there(p, wait)

    def retire(refs, turn):
        for i in range(pieces):
            if_there(sends[i][0], lambda: copy(i, *refs, turn).wait_send())

    def pick(tiles, firsts, index):
        shape = tiles[0].shape
        lane = jnp.broadcast_to(index & (LANES - 1), shape)
        tile = jnp.broadcast_to(index >> 7, shape)
        out = jnp.zeros(shape, tiles[0].dtype)
        for values, first in zip(tiles, firsts):
            moved = jnp.take_along_axis(values, lane, axis=1, mode="promise_in_bounds")
            out = jnp.where(tile == first, moved, out)
        return out

    def own_part(tiles):
        return tiles, range(len(tiles))

    def halo_part(land, turn, group, own):
        slots = [member_of(p, q) for p, q in group]
        return [land[turn, slot] for slot in slots], [own + slot for slot in slots]

    def edge_columns(ref, row, k):
        stop = min(edges, (k + 1) * LANES)
        part = row(ref)[:, k * LANES : stop]
        short = (k + 1) * LANES - stop
        return jnp.pad(part, ((0, 0), (0, short))) if short else part

    def span(i):
        return slice(i * rows, (i + 1) * rows)

    def listed(row_tiles, index):
        shape = (pieces, LANES)
        tiles = [jnp.broadcast_to(tile, shape) for tile in row_tiles]
        return pick(tiles, range(len(tiles)), index)

    def piece_change(i, part):
        low, high = (pick(*part, ec_list[r, i : i + 1, :]) for r in (0, 1))
        return high - low

    def piece_sum(i, part):
        total = None
        for j in range(3):
            term = pick(*part, ce_list[j, i : i + 1, :]) * weight_list[j, i : i + 1, :]
            total = term if total is None else total + term
        return total

    def add_gradient(part, fresh, last):
        for k in range(ecols // LANES):
            cols = slice(k * LANES, (k + 1) * LANES)
            taken = [
                pick(*part, spread(edge_columns(ec, lambda ref: ref[0, r : r + 1, :], k), cells, ccols))
                for r in (0, 1)
            ]
            change = taken[1] - taken[0]
            total = change if fresh else grad[:, cols] + change
            if last:
                scale = step_scale * edge_columns(inv_dual, lambda ref: ref[...], k)
                vf[:, cols] = vf[:, cols] - scale * total
            else:
                grad[:, cols] = total

    def add_divergence(part, fresh, last):
        for k in range(ccols // LANES):
            cols = slice(k * LANES, (k + 1) * LANES)
            total = None if fresh else div[:, cols]
            for j in range(3):
                term = pick(*part, spread(ce[j, :, cols], edges, ecols)) * weight[j, :, cols]
                total = term if total is None else total + term
            if last:
                right = pf[:, cols] - sound[:, cols] * total
                work[0:nlev, cols] = right[0:nlev] * t_inv[:, cols]
            else:
                div[:, cols] = total

    def eliminate(couple, put):
        ups = {}
        for k in [*range(middle), *range(nlev - 1, middle - 1, -1)]:
            here, below_it = couple(k), couple(k - 1) if k else None
            diagonal = 1.0 + here if k == 0 else 1.0 + below_it + here
            toward, away = (here, below_it) if k < middle else (below_it, here)
            last = ups.get(k - 1 if k < middle else k + 1)
            inverse = 1.0 / (diagonal if last is None else diagonal - away * last)
            ups[k] = toward * inverse
            put(k, inverse, None if last is None else away * inverse, ups[k])
        return 1.0 / (1.0 - ups[middle - 1] * ups[middle])

    def sweep(scaled, low, up, mid, hold, held, put):
        top = bottom = None
        for step in range(max(middle, nlev - middle)):
            k = step
            if k < middle:
                top = scaled(k) if top is None else scaled(k) + low(k) * top
                hold(k, top)
            k = nlev - 1 - step
            if k >= middle:
                bottom = scaled(k) if bottom is None else scaled(k) + low(k) * bottom
                hold(k, bottom)
        bottom = (bottom + up(middle) * top) * mid
        top = top + up(middle - 1) * bottom
        put(middle, bottom)
        put(middle - 1, top)
        for step in range(1, max(middle, nlev - middle)):
            k = middle - 1 - step
            if k >= 0:
                top = held(k) + up(k) * top
                put(k, top)
            k = middle + step
            if k < nlev:
                bottom = held(k) + up(k) * bottom
                put(k, bottom)

    def level(k):
        return slice(k, k + 1)

    def across(k, batch):
        return pl.ds(k + batch.start * rows, len(batch), stride=rows)

    def own_columns():
        def put(k, inverse, low, up):
            t_inv[level(k), :] = inverse
            t_up[level(k), :] = up
            if low is not None:
                t_low[level(k), :] = low
        t_mid[...] = eliminate(lambda k: coupling[k], put)

    def piece_columns():
        for k in range(nlev):
            work[level(k), :] = coupling[k]
        tiles = own_part(tiles_of(work, ccols))
        for i in range(pieces):
            s_div[span(i), :] = pick(*tiles, sc_list[i : i + 1, :])

        def put(k, inverse, low, up):
            s_inv[k] = inverse
            s_up[k] = up
            if low is not None:
                s_low[k] = low
        s_mid[...] = eliminate(lambda k: s_div[across(k, range(pieces)), :], put)

    def solve_pieces(batch):
        kept = {}
        some = slice(batch.start, batch.stop)

        def put(k, value):
            p_send[across(k, batch), :] = value
        sweep(
            lambda k: s_div[across(k, batch), :] * s_inv[k, some], lambda k: s_low[k, some],
            lambda k: s_up[k, some], s_mid[some, :], kept.__setitem__, kept.__getitem__, put,
        )

    def solve_own(put):
        def hold(k, value):
            work[level(k), :] = value
        sweep(
            lambda k: work[level(k), :], lambda k: t_low[level(k), :], lambda k: t_up[level(k), :], t_mid[...],
            hold, lambda k: work[level(k), :], put,
        )

    p_refs = (p_send, p_halo, p_ss, p_rs)
    v_refs = (v_send, v_halo, v_ss, v_rs)
    for load in loads[:2]:
        load.wait()
    for k in range(nlev):
        pf[level(k), :] = p_row[k]
    for i, offset in enumerate(sends):
        sc_list[i : i + 1, :] = sc[0, pl.ds(member_of(*offset), 1), :]
    own = own_part(tiles_of(pf, ccols))
    for i in range(pieces):
        p_send[span(i), :] = pick(*own, sc_list[i : i + 1, :])
    bands = (a + n_lat - 1) // n_lat + (2 * n_lat - 2 - a) // n_lat
    pl.semaphore_wait(barrier, 2 + 3 * bands)
    launch(range(pieces), p_refs, 0)

    for load in loads[2:]:
        load.wait()
    for k in range(nlev):
        vf[level(k), 0:edges] = v_row[k]
    for i, offset in enumerate(sends):
        se_list[i : i + 1, :] = se[0, pl.ds(member_of(*offset), 1), :]
    blocks = range(ecols // LANES)
    index = se_list[...]
    for r in (0, 1):
        row = [edge_columns(ec, lambda ref: ref[0, r : r + 1, :], k) for k in blocks]
        ec_list[r] = spread(listed(row, index), cells, ccols)
    scale_list[...] = step_scale * listed([edge_columns(inv_dual, lambda ref: ref[...], k) for k in blocks], index)
    own = own_part(tiles_of(vf, ecols))
    for i in range(pieces):
        v_send[span(i), :] = pick(*own, se_list[i : i + 1, :])

    def compose_cells():
        index = sc_list[...]
        cuts = [slice(k * LANES, (k + 1) * LANES) for k in range(ccols // LANES)]
        for j in range(3):
            ce_list[j] = spread(listed([ce[j, :, cut] for cut in cuts], index), edges, ecols)
            weight_list[j] = listed([weight[j, :, cut] for cut in cuts], index)
        sound_list[...] = listed([sound[:, cut] for cut in cuts], index)

    for substep in range(NSUB):
        final = substep == NSUB - 1
        turn = substep % 2
        own = own_part(tiles_of(pf, ccols))
        for i in range(pieces):
            s_grad[span(i), :] = piece_change(i, own)
        add_gradient(own, True, False)
        if substep == 0:
            compose_cells()
            piece_columns()
            own_columns()
        else:
            retire(v_refs, 1 - turn)
        arrive(sends, p_refs, turn)
        part = halo_part(p_halo, turn, sends, ccols // LANES)
        for batch in v_batches:
            for i in batch:
                change = s_grad[span(i), :] + piece_change(i, part)
                v_send[span(i), :] = v_send[span(i), :] - scale_list[i : i + 1, :] * change
            launch(batch, v_refs, turn)
        add_gradient(part, False, True)
        if final:
            for k in range(nlev):
                v_out[k] = vf[level(k), 0:edges]

        own = own_part(tiles_of(vf, ecols))
        if not final:
            for i in range(pieces):
                s_div[span(i), :] = piece_sum(i, own)
        add_divergence(own, True, False)
        retire(p_refs, turn)
        arrive(sends, v_refs, turn)
        part = halo_part(v_halo, turn, sends, ecols // LANES)
        if final:
            def put(k, value):
                p_out[k] = value
        else:
            for batch in p_batches:
                for i in batch:
                    total = s_div[span(i), :] + piece_sum(i, part)
                    s_div[span(i), :] = p_send[span(i), :] - sound_list[i : i + 1, :] * total
                solve_pieces(batch)
                launch(batch, p_refs, 1 - turn)

            def put(k, value):
                pf[level(k), :] = value
        add_divergence(part, False, True)
        solve_own(put)

    retire(v_refs, turn)


def write_out(p_ref, v_ref, p_out, v_out, sem):
    stores = [
        pltpu.make_async_copy(x, y, sem.at[k])
        for k, (x, y) in enumerate(((v_ref, v_out), (p_ref, p_out)))
    ]
    for store in stores:
        store.start()
    for store in stores:
        store.wait()


def level_major(x):
    return jnp.transpose(x, (1, 0, 2))


def on_device(*args):
    pressure, velocity, send_cells = args[0], args[1], args[4]
    n_lat, n_lon = lax.axis_size("lat"), lax.axis_size("lon")
    nlev, cells, edges = pressure.shape[1], pressure.shape[2], velocity.shape[2]
    halo = send_cells.shape[2]
    rows, ecols = round_up(nlev, 32), round_up(edges, 128)
    hbm = pl.BlockSpec(memory_space=pltpu.HBM)
    vmem = pl.BlockSpec(memory_space=pltpu.VMEM)
    dma8 = pltpu.SemaphoreType.DMA((8,))
    args = [level_major(x) if k in (0, 1, 3, 7, 9) else x for k, x in enumerate(args)]

    def body(*refs):
        kernel(n_lat, n_lon, nlev, cells, edges, halo, *refs)

    halo_shape = pltpu.VMEM((2, 8, rows, halo), F32)
    piece_shape = pltpu.VMEM((8 * rows, halo), F32)
    list_shape = pltpu.VMEM((8, halo), F32)
    places = pltpu.VMEM((8, halo), jnp.int32)
    cell_shape = pltpu.VMEM((rows, cells), F32)
    edge_shape = pltpu.VMEM((rows, ecols), F32)
    level_shape = pltpu.VMEM((nlev, cells), F32)
    stack_shape = pltpu.VMEM((nlev, 8, halo), F32)
    outs = pl.pallas_call(
        body,
        name="substeps",
        out_shape=(
            pltpu.VMEM(args[0].shape, F32),
            pltpu.VMEM(args[1].shape, F32),
        ),
        in_specs=[hbm] * len(args),
        out_specs=(vmem, vmem),
        scratch_shapes=[pltpu.VMEM(x.shape, x.dtype) for x in args] + [
            cell_shape, edge_shape, piece_shape, piece_shape, halo_shape, halo_shape,
            level_shape, level_shape, level_shape, pltpu.VMEM((1, cells), F32), cell_shape, edge_shape, cell_shape,
            places, places, pltpu.VMEM((2, 8, halo), jnp.int32), pltpu.VMEM((3, 8, halo), jnp.int32),
            list_shape, pltpu.VMEM((3, 8, halo), F32), list_shape,
            stack_shape, stack_shape, stack_shape, list_shape, piece_shape, piece_shape,
            dma8, dma8, dma8, dma8,
            pltpu.SemaphoreType.DMA((len(args),)),
        ],
        compiler_params=pltpu.CompilerParams(
            collective_id=0, has_side_effects=True, vmem_limit_bytes=66_000_000
        ),
    )(*args)
    outs = pl.pallas_call(
        write_out,
        name="write_out",
        out_shape=tuple(jax.ShapeDtypeStruct(x.shape, F32) for x in outs),
        in_specs=[vmem] * 2,
        out_specs=(hbm, hbm),
        scratch_shapes=[pltpu.SemaphoreType.DMA((2,))],
        compiler_params=pltpu.CompilerParams(vmem_limit_bytes=1024 * 1024),
    )(*outs)
    return tuple(level_major(x) for x in outs)


def solution(mesh):
    band = P("lat", None, "lon")
    flat = P("lat", "lon")
    return jax.shard_map(
        on_device,
        mesh=mesh,
        in_specs=(band, band, band, band, band, band, flat, band, flat, band),
        out_specs=(band, band),
        check_vma=False,
    )
```

```python
import math

import jax
import jax.numpy as jnp
from jax import lax
from jax.experimental import pallas as pl
from jax.experimental.pallas import tpu as pltpu
from jax.sharding import PartitionSpec as P

NSUB = 3
OFFSETS = ((-1, -1), (-1, 0), (-1, 1), (0, -1), (0, 1), (1, -1), (1, 0), (1, 1))
LANES = 128
step_scale = 0.5
MESH = pl.DeviceIdType.MESH
F32 = jnp.float32


def round_up(n, m):
    return (n + m - 1) // m * m


def tiles_of(ref, width):
    return [ref[:, k * LANES : (k + 1) * LANES] for k in range(width // LANES)]


def spread(index, own, padded):
    return jnp.where(index >= own, index + (padded - own), index)


def member_of(p, q):
    if isinstance(p, int) and p == 0:
        return 3 + (q + 1) // 2
    return (7 + 5 * p) // 2 + q


def kernel(
    n_lat, n_lon, nlev, cells, edges, halo,
    p_hbm, v_hbm, ec_hbm, ce_hbm, sc_hbm, se_hbm, inv_hbm, weight_hbm, sound_hbm, coupling_hbm,
    p_out, v_out,
    p_home, v_home, ec_home, ce_home, sc_home, se_home, inv_home, weight_home, sound_home, coupling_home,
    p_row, v_row, ec, ce, sc, se, inv_dual, weight, sound, coupling,
    pf, vf, pf_home, vf_home, h_send, p_send, v_send, p_halo, v_halo,
    t_inv, t_low, t_up, t_mid, work, grad, div,
    sc_list, se_list, ec_list, ce_list, scale_list, weight_list, sound_list,
    s_inv, s_low, s_up, s_mid, s_grad, s_div,
    p_ss, p_rs, v_ss, v_rs, f_rs, in_sem, work_sem,
):
    a, home = lax.axis_index("lat"), lax.axis_index("lon")
    chips = n_lon // 2
    chip, core = home // 2, lax.rem(home, 2)
    partner = home + 1 - 2 * core
    traded = chip < chips // 2
    b = jnp.where(traded, partner, home)
    ccols, ecols = pf.shape[1], vf.shape[1]
    rows = pf.shape[0]
    pieces = len(OFFSETS)
    middle = nlev // 2
    side = math.isqrt(n_lat)
    slow = jnp.where(lax.rem(a, side) == side - 1, 1, -1)
    quick = -slow

    def ordered(far):
        near = -far
        return [
            (slow, far), (slow, near), (slow, 0), (quick, far), (0, far),
            (quick, near), (quick, 0), (0, near),
        ]

    home_sends = ordered(2 * core - 1)
    sends = ordered(2 * lax.rem(b, 2) - 1)
    p_batches = (range(0, 2), range(2, 5), range(5, 8),)
    v_batches = (range(0, 2), range(2, 5), range(5, 8),)

    def if_there(p, fn):
        if isinstance(p, int) and p == 0:
            fn()
        else:
            pl.when((a + p >= 0) & (a + p < n_lat))(fn)

    def around(sector, q):
        return lax.rem(sector + q + n_lon, n_lon)

    def worker(sector):
        return jnp.where(sector < 2 * (chips // 2), sector + 1 - 2 * lax.rem(sector, 2), sector)

    loads = [
        pltpu.make_async_copy(x, y, in_sem.at[k])
        for k, (x, y) in enumerate(((p_hbm, p_home), (sc_hbm, sc_home)))
    ]
    for load in loads:
        load.start()

    bands = (a + n_lat - 1) // n_lat + (2 * n_lat - 2 - a) // n_lat
    barrier = pltpu.get_barrier_semaphore()
    across_out = around(b, 2 * lax.rem(b, 2) - 1)
    across_home = around(home, 2 * core - 1)
    doubled = across_out < 2 * (chips // 2)
    for lat_step in (-1, 1, 0):
        def greet(lat_step=lat_step):
            def signal(sector):
                pl.semaphore_signal(
                    barrier, inc=1, device_id=(a + lat_step, sector), device_id_type=MESH
                )
            signal(across_out)
            pl.when(doubled)(lambda: signal(worker(across_out)))
            pl.when(traded)(lambda: signal(worker(across_home)))
            signal(partner)
            if lat_step != 0:
                signal(home)
        if_there(lat_step, greet)

    kept = [p_home, sc_home, ec_home, v_home, se_home, inv_home, coupling_home, ce_home, weight_home, sound_home]
    held = [p_row, sc, ec, v_row, se, inv_dual, coupling, ce, weight, sound]
    given = [p_hbm, sc_hbm, ec_hbm, v_hbm, se_hbm, inv_hbm, coupling_hbm, ce_hbm, weight_hbm, sound_hbm]
    loads += [
        pltpu.make_async_copy(x, y, in_sem.at[k + 2]) for k, (x, y) in enumerate(zip(given[2:], kept[2:]))
    ]
    fills = [pltpu.make_async_copy(x, y, work_sem.at[k]) for k, (x, y) in enumerate(zip(given, held))]
    gifts = [
        pltpu.make_async_remote_copy(
            src_ref=x, dst_ref=y, send_sem=in_sem.at[k], recv_sem=work_sem.at[k],
            device_id=(a, partner), device_id_type=MESH,
        )
        for k, (x, y) in enumerate(zip(kept, held))
    ]
    returns = [
        pltpu.make_async_remote_copy(
            src_ref=x, dst_ref=y, send_sem=in_sem.at[k], recv_sem=work_sem.at[k],
            device_id=(a, partner), device_id_type=MESH,
        )
        for k, (x, y) in enumerate(((pf, pf_home), (vf, vf_home)))
    ]
    for load in loads[2:]:
        load.start()

    @pl.when(jnp.logical_not(traded))
    def _():
        for fill in fills:
            fill.start()

    def clear(p):
        def fill():
            for slot, offset in enumerate(OFFSETS):
                if offset[0] == p:
                    for turn in range(2):
                        p_halo[turn, slot] = jnp.zeros(p_halo.shape[2:], F32)
                    for turn in range(NSUB):
                        v_halo[turn, slot] = jnp.zeros(v_halo.shape[2:], F32)
        return fill

    pl.when(a == 0)(clear(-1))
    pl.when(a == n_lat - 1)(clear(1))
    pf[nlev - nlev % 8 :, :] = jnp.zeros_like(pf[nlev - nlev % 8 :, :])
    work[nlev - nlev % 8 :, :] = jnp.zeros_like(pf[nlev - nlev % 8 :, :])
    vf[...] = jnp.zeros_like(vf)

    def copy(i, route, send, land, ss, rs, turn):
        offsets, sector, place = route
        p, q = offsets[i]
        member = member_of(p, q)
        return pltpu.make_async_remote_copy(
            src_ref=send.at[pl.ds(i * rows, rows)], dst_ref=land.at[turn, 7 - member],
            send_sem=ss.at[0], recv_sem=rs.at[0],
            device_id=(a + p, place(around(sector, q))), device_id_type=MESH,
        )

    out_route = (home_sends, home, worker)
    mid_route = (sends, b, worker)
    back_route = (sends, b, lambda sector: sector)
    local = pieces - 1

    def stays(i, route, fn):
        if i == local and route is not mid_route:
            pl.when(jnp.logical_not(traded))(fn)
        else:
            if_there(sends[i][0], fn)

    def launch(batch, route, refs, turn):
        for i in batch:
            stays(i, route, lambda: copy(i, route, *refs, turn).start())
            if i == local and route is not mid_route:
                send, land = refs[:2]
                slot = 7 - member_of(*route[0][i])

                @pl.when(traded)
                def _():
                    land[turn, slot] = send[span(i), :]

    def settle(route, refs, fn):
        send, _, ss, rs = refs
        numbers = {2 + 3 * n for n in ((1, 2) if n_lat > 2 else (n_lat - 1,))}
        total = 2 + 3 * bands
        if route is not mid_route:
            numbers |= {n - 1 for n in numbers}
            total = total - traded.astype(jnp.int32)
        for n in sorted(numbers):
            whole = send.at[pl.ds(0, n * rows)]
            both = pltpu.make_async_remote_copy(
                src_ref=whole, dst_ref=whole, send_sem=ss.at[0], recv_sem=rs.at[0],
                device_id=(a, partner), device_id_type=MESH,
            )
            pl.when(total == n)(lambda: fn(both))

    def arrive(route, refs):
        settle(route, refs, lambda copies: copies.wait_recv())

    def retire(route, refs):
        settle(route, refs, lambda copies: copies.wait_send())

    def pick(tiles, firsts, index):
        shape = tiles[0].shape
        lane = jnp.broadcast_to(index & (LANES - 1), shape)
        tile = jnp.broadcast_to(index >> 7, shape)
        out = jnp.zeros(shape, tiles[0].dtype)
        for values, first in zip(tiles, firsts):
            moved = jnp.take_along_axis(values, lane, axis=1, mode="promise_in_bounds")
            out = jnp.where(tile == first, moved, out)
        return out

    def own_part(tiles):
        return tiles, range(len(tiles))

    def halo_part(land, turn, group, own):
        slots = [member_of(p, q) for p, q in group]
        return [land[turn, slot] for slot in slots], [own + slot for slot in slots]

    def edge_columns(ref, row, k):
        stop = min(edges, (k + 1) * LANES)
        part = row(ref)[:, k * LANES : stop]
        short = (k + 1) * LANES - stop
        return jnp.pad(part, ((0, 0), (0, short))) if short else part

    def span(i):
        return slice(i * rows, (i + 1) * rows)

    def listed(row_tiles, index):
        shape = (pieces, LANES)
        tiles = [jnp.broadcast_to(tile, shape) for tile in row_tiles]
        return pick(tiles, range(len(tiles)), index)

    def piece_change(i, part):
        low, high = (pick(*part, ec_list[r, i : i + 1, :]) for r in (0, 1))
        return high - low

    def piece_sum(i, part):
        total = None
        for j in range(3):
            term = pick(*part, ce_list[j, i : i + 1, :]) * weight_list[j, i : i + 1, :]
            total = term if total is None else total + term
        return total

    def add_gradient(part, fresh, last):
        for k in range(ecols // LANES):
            cols = slice(k * LANES, (k + 1) * LANES)
            taken = [
                pick(*part, spread(edge_columns(ec, lambda ref: ref[0, r : r + 1, :], k), cells, ccols))
                for r in (0, 1)
            ]
            change = taken[1] - taken[0]
            total = change if fresh else grad[:, cols] + change
            if last:
                scale = step_scale * edge_columns(inv_dual, lambda ref: ref[...], k)
                vf[:, cols] = vf[:, cols] - scale * total
            else:
                grad[:, cols] = total

    def add_divergence(part, fresh, last, sides, factors, speeds, values):
        for k in range(ccols // LANES):
            cols = slice(k * LANES, (k + 1) * LANES)
            total = None if fresh else div[:, cols]
            for j in range(3):
                term = pick(*part, spread(sides[j, :, cols], edges, ecols)) * factors[j, :, cols]
                total = term if total is None else total + term
            if last:
                right = values[:, cols] - speeds[:, cols] * total
                work[0:nlev, cols] = right[0:nlev] * t_inv[:, cols]
            else:
                div[:, cols] = total

    def eliminate(couple, put):
        ups = {}
        for k in [*range(middle), *range(nlev - 1, middle - 1, -1)]:
            here, below_it = couple(k), couple(k - 1) if k else None
            diagonal = 1.0 + here if k == 0 else 1.0 + below_it + here
            toward, away = (here, below_it) if k < middle else (below_it, here)
            last = ups.get(k - 1 if k < middle else k + 1)
            inverse = 1.0 / (diagonal if last is None else diagonal - away * last)
            ups[k] = toward * inverse
            put(k, inverse, None if last is None else away * inverse, ups[k])
        return 1.0 / (1.0 - ups[middle - 1] * ups[middle])

    def sweep(scaled, low, up, mid, hold, held, put):
        top = bottom = None
        for step in range(max(middle, nlev - middle)):
            k = step
            if k < middle:
                top = scaled(k) if top is None else scaled(k) + low(k) * top
                hold(k, top)
            k = nlev - 1 - step
            if k >= middle:
                bottom = scaled(k) if bottom is None else scaled(k) + low(k) * bottom
                hold(k, bottom)
        bottom = (bottom + up(middle) * top) * mid
        top = top + up(middle - 1) * bottom
        put(middle, bottom)
        put(middle - 1, top)
        for step in range(1, max(middle, nlev - middle)):
            k = middle - 1 - step
            if k >= 0:
                top = held(k) + up(k) * top
                put(k, top)
            k = middle + step
            if k < nlev:
                bottom = held(k) + up(k) * bottom
                put(k, bottom)

    def level(k):
        return slice(k, k + 1)

    def across(k, batch):
        return pl.ds(k + batch.start * rows, len(batch), stride=rows)

    def own_columns(coupling):
        def put(k, inverse, low, up):
            t_inv[level(k), :] = inverse
            t_up[level(k), :] = up
            if low is not None:
                t_low[level(k), :] = low
        t_mid[...] = eliminate(lambda k: coupling[k], put)

    def piece_columns():
        for k in range(nlev):
            work[level(k), :] = coupling[k]
        tiles = own_part(tiles_of(work, ccols))
        for i in range(pieces):
            s_div[span(i), :] = pick(*tiles, sc_list[i : i + 1, :])

        def put(k, inverse, low, up):
            s_inv[k] = inverse
            s_up[k] = up
            if low is not None:
                s_low[k] = low
        s_mid[...] = eliminate(lambda k: s_div[across(k, range(pieces)), :], put)

    def solve_pieces(batch):
        kept = {}
        some = slice(batch.start, batch.stop)

        def put(k, value):
            p_send[across(k, batch), :] = value
        sweep(
            lambda k: s_div[across(k, batch), :] * s_inv[k, some], lambda k: s_low[k, some],
            lambda k: s_up[k, some], s_mid[some, :], kept.__setitem__, kept.__getitem__, put,
        )

    def solve_own(put):
        def hold(k, value):
            work[level(k), :] = value
        sweep(
            lambda k: work[level(k), :], lambda k: t_low[level(k), :], lambda k: t_up[level(k), :], t_mid[...],
            hold, lambda k: work[level(k), :], put,
        )

    h_refs = (h_send, p_halo, p_ss, p_rs)
    p_refs = (p_send, p_halo, p_ss, p_rs)
    v_refs = (v_send, v_halo, v_ss, v_rs)
    f_refs = (v_send, v_halo, v_ss, f_rs)
    for load in loads[:2]:
        load.wait()
    for k in range(nlev):
        pf[level(k), :] = p_home[k]
    own = own_part(tiles_of(pf, ccols))
    for i, offset in enumerate(home_sends):
        h_send[span(i), :] = pick(*own, sc_home[0, pl.ds(member_of(*offset), 1), :])
    reached = 2 + doubled.astype(jnp.int32) + traded.astype(jnp.int32)
    pl.semaphore_wait(barrier, reached + (reached + 1) * bands)
    launch(range(pieces), out_route, h_refs, 0)
    for load in loads[2:]:
        load.wait()

    @pl.when(traded)
    def _():
        for gift in gifts:
            gift.start()
        for gift in gifts:
            gift.wait_recv()

    @pl.when(jnp.logical_not(traded))
    def _():
        for fill in fills:
            fill.wait()

    for k in range(nlev):
        pf[level(k), :] = p_row[k]
        vf[level(k), 0:edges] = v_row[k]
    for i, offset in enumerate(sends):
        sc_list[i : i + 1, :] = sc[0, pl.ds(member_of(*offset), 1), :]
        se_list[i : i + 1, :] = se[0, pl.ds(member_of(*offset), 1), :]
    own = own_part(tiles_of(pf, ccols))
    for i in range(pieces):
        p_send[span(i), :] = pick(*own, sc_list[i : i + 1, :])
    blocks = range(ecols // LANES)
    index = se_list[...]
    for r in (0, 1):
        row = [edge_columns(ec, lambda ref: ref[0, r : r + 1, :], k) for k in blocks]
        ec_list[r] = spread(listed(row, index), cells, ccols)
    scale_list[...] = step_scale * listed([edge_columns(inv_dual, lambda ref: ref[...], k) for k in blocks], index)
    own = own_part(tiles_of(vf, ecols))
    for i in range(pieces):
        v_send[span(i), :] = pick(*own, se_list[i : i + 1, :])

    def compose_cells():
        index = sc_list[...]
        cuts = [slice(k * LANES, (k + 1) * LANES) for k in range(ccols // LANES)]
        for j in range(3):
            ce_list[j] = spread(listed([ce[j, :, cut] for cut in cuts], index), edges, ecols)
            weight_list[j] = listed([weight[j, :, cut] for cut in cuts], index)
        sound_list[...] = listed([sound[:, cut] for cut in cuts], index)

    here = (ce, weight, sound, pf)
    for substep in range(NSUB):
        final = substep == NSUB - 1
        turn = substep % 2
        route = mid_route if substep else out_route
        own = own_part(tiles_of(pf, ccols))
        for i in range(pieces):
            s_grad[span(i), :] = piece_change(i, own)
        add_gradient(own, True, False)
        if substep == 0:
            compose_cells()
            piece_columns()
            own_columns(coupling)
        else:
            retire(mid_route, v_refs)
        arrive(route, p_refs)
        part = halo_part(p_halo, turn, sends, ccols // LANES)
        for batch in v_batches:
            for i in batch:
                change = s_grad[span(i), :] + piece_change(i, part)
                v_send[span(i), :] = v_send[span(i), :] - scale_list[i : i + 1, :] * change
            if final:
                launch(batch, back_route, f_refs, substep)
            else:
                launch(batch, mid_route, v_refs, substep)
        add_gradient(part, False, True)
        if final:
            pl.when(traded)(returns[1].start)
            pl.when(traded)(lambda: own_columns(coupling_home))
            pl.when(traded)(returns[0].wait_recv)
            pl.when(traded)(returns[1].wait_recv)

            @pl.when(jnp.logical_not(traded))
            def _():
                pf_home[...] = pf[...]
                vf_home[...] = vf[...]

            for k in range(nlev):
                v_out[k] = vf_home[level(k), 0:edges]
            own = own_part(tiles_of(vf_home, ecols))
            here = (ce_home, weight_home, sound_home, pf_home)
        else:
            own = own_part(tiles_of(vf, ecols))
            for i in range(pieces):
                s_div[span(i), :] = piece_sum(i, own)
        add_divergence(own, True, False, *here)
        if substep in (0, NSUB - 1):
            sent = returns if final else gifts
            pl.when(traded)(lambda: [x.wait_send() for x in sent] and None)

        retire(route, h_refs if substep == 0 else p_refs)
        if final:
            arrive(back_route, f_refs)
            part = halo_part(v_halo, substep, home_sends, ecols // LANES)

            def put(k, value):
                p_out[k] = value
        else:
            arrive(mid_route, v_refs)
            part = halo_part(v_halo, substep, sends, ecols // LANES)
            for batch in p_batches:
                for i in batch:
                    total = s_div[span(i), :] + piece_sum(i, part)
                    s_div[span(i), :] = p_send[span(i), :] - sound_list[i : i + 1, :] * total
                solve_pieces(batch)
                launch(batch, mid_route, p_refs, 1 - turn)

            def put(k, value):
                pf[level(k), :] = value
        add_divergence(part, False, True, *here)
        solve_own(put)
        if substep == NSUB - 2:
            pl.when(traded)(returns[0].start)

    retire(back_route, f_refs)


def write_out(p_ref, v_ref, p_out, v_out, sem):
    stores = [
        pltpu.make_async_copy(x, y, sem.at[k])
        for k, (x, y) in enumerate(((v_ref, v_out), (p_ref, p_out)))
    ]
    for store in stores:
        store.start()
    for store in stores:
        store.wait()


def level_major(x):
    return jnp.transpose(x, (1, 0, 2))


def on_device(*args):
    pressure, velocity, send_cells = args[0], args[1], args[4]
    n_lat, n_lon = lax.axis_size("lat"), lax.axis_size("lon")
    nlev, cells, edges = pressure.shape[1], pressure.shape[2], velocity.shape[2]
    halo = send_cells.shape[2]
    rows, ecols = round_up(nlev, 32), round_up(edges, 128)
    hbm = pl.BlockSpec(memory_space=pltpu.HBM)
    vmem = pl.BlockSpec(memory_space=pltpu.VMEM)
    args = [level_major(x) if k in (0, 1, 3, 7, 9) else x for k, x in enumerate(args)]

    def body(*refs):
        kernel(n_lat, n_lon, nlev, cells, edges, halo, *refs)

    halo_shape = pltpu.VMEM((2, 8, rows, halo), F32)
    piece_shape = pltpu.VMEM((8 * rows, halo), F32)
    list_shape = pltpu.VMEM((8, halo), F32)
    places = pltpu.VMEM((8, halo), jnp.int32)
    cell_shape = pltpu.VMEM((rows, cells), F32)
    edge_shape = pltpu.VMEM((rows, ecols), F32)
    level_shape = pltpu.VMEM((nlev, cells), F32)
    stack_shape = pltpu.VMEM((nlev, 8, halo), F32)
    outs = pl.pallas_call(
        body,
        name="substeps",
        out_shape=(
            pltpu.VMEM(args[0].shape, F32),
            pltpu.VMEM(args[1].shape, F32),
        ),
        in_specs=[hbm] * len(args),
        out_specs=(vmem, vmem),
        scratch_shapes=[pltpu.VMEM(x.shape, x.dtype) for x in args] * 2 + [
            cell_shape, edge_shape, cell_shape, edge_shape, piece_shape, piece_shape, piece_shape,
            halo_shape, pltpu.VMEM((NSUB, 8, rows, halo), F32),
            level_shape, level_shape, level_shape, pltpu.VMEM((1, cells), F32), cell_shape, edge_shape, cell_shape,
            places, places, pltpu.VMEM((2, 8, halo), jnp.int32), pltpu.VMEM((3, 8, halo), jnp.int32),
            list_shape, pltpu.VMEM((3, 8, halo), F32), list_shape,
            stack_shape, stack_shape, stack_shape, list_shape, piece_shape, piece_shape,
            *[pltpu.SemaphoreType.DMA((1,))] * 5,
            *[pltpu.SemaphoreType.DMA((len(args),))] * 2,
        ],
        compiler_params=pltpu.CompilerParams(
            collective_id=0, has_side_effects=True, vmem_limit_bytes=66_000_000
        ),
    )(*args)
    outs = pl.pallas_call(
        write_out,
        name="write_out",
        out_shape=tuple(jax.ShapeDtypeStruct(x.shape, F32) for x in outs),
        in_specs=[vmem] * 2,
        out_specs=(hbm, hbm),
        scratch_shapes=[pltpu.SemaphoreType.DMA((2,))],
        compiler_params=pltpu.CompilerParams(vmem_limit_bytes=1024 * 1024),
    )(*outs)
    return tuple(level_major(x) for x in outs)


def solution(mesh):
    band = P("lat", None, "lon")
    flat = P("lat", "lon")
    return jax.shard_map(
        on_device,
        mesh=mesh,
        in_specs=(band, band, band, band, band, band, flat, band, flat, band),
        out_specs=(band, band),
        check_vma=False,
    )
```

```python
import math

import jax
import jax.numpy as jnp
from jax import lax
from jax.experimental import pallas as pl
from jax.experimental.pallas import tpu as pltpu
from jax.sharding import PartitionSpec as P

NSUB = 3
OFFSETS = ((-1, -1), (-1, 0), (-1, 1), (0, -1), (0, 1), (1, -1), (1, 0), (1, 1))
LANES = 128
step_scale = 0.5
MESH = pl.DeviceIdType.MESH
F32 = jnp.float32


def round_up(n, m):
    return (n + m - 1) // m * m


def tiles_of(ref, width):
    return [ref[:, k * LANES : (k + 1) * LANES] for k in range(width // LANES)]


def spread(index, own, padded):
    return jnp.where(index >= own, index + (padded - own), index)


def member_of(p, q):
    if isinstance(p, int) and p == 0:
        return 3 + (q + 1) // 2
    return (7 + 5 * p) // 2 + q


def kernel(
    n_lat, n_lon, nlev, cells, edges, halo,
    p_hbm, v_hbm, ec_hbm, ce_hbm, sc_hbm, se_hbm, inv_hbm, weight_hbm, sound_hbm, coupling_hbm,
    p_out, v_out,
    p_home, v_home, ec_home, ce_home, sc_home, se_home, inv_home, weight_home, sound_home, coupling_home,
    p_row, v_row, ec, ce, sc, se, inv_dual, weight, sound, coupling,
    pf, vf, pf_home, vf_home, h_send, p_send, v_send, p_halo, v_halo,
    t_inv, t_low, t_up, t_mid, work, grad, div,
    sc_list, se_list, ec_list, ce_list, scale_list, weight_list, sound_list,
    s_inv, s_low, s_up, s_mid, s_grad, s_div,
    p_ss, p_rs, v_ss, v_rs, f_rs, in_sem, work_sem,
):
    a, home = lax.axis_index("lat"), lax.axis_index("lon")
    chips = n_lon // 2
    chip, core = home // 2, lax.rem(home, 2)
    partner = home + 1 - 2 * core
    traded = chip < chips // 2
    b = jnp.where(traded, partner, home)
    ccols, ecols = pf.shape[1], vf.shape[1]
    rows = pf.shape[0]
    pieces = len(OFFSETS)
    middle = nlev // 2
    side = math.isqrt(n_lat)
    slow = jnp.where(lax.rem(a, side) == side - 1, 1, -1)
    quick = -slow

    def ordered(far):
        near = -far
        return [
            (slow, far), (slow, near), (slow, 0), (quick, far), (0, far),
            (quick, near), (quick, 0), (0, near),
        ]

    home_sends = ordered(2 * core - 1)
    sends = ordered(2 * lax.rem(b, 2) - 1)
    p_batches = (range(0, 2), range(2, 4), range(4, 6), range(6, 8),)
    v_batches = (range(0, 2), range(2, 4), range(4, 6), range(6, 8),)

    def if_there(p, fn):
        if isinstance(p, int) and p == 0:
            fn()
        else:
            pl.when((a + p >= 0) & (a + p < n_lat))(fn)

    def around(sector, q):
        return lax.rem(sector + q + n_lon, n_lon)

    def worker(sector):
        return jnp.where(sector < 2 * (chips // 2), sector + 1 - 2 * lax.rem(sector, 2), sector)

    loads = [
        pltpu.make_async_copy(x, y, in_sem.at[k])
        for k, (x, y) in enumerate(((p_hbm, p_home), (sc_hbm, sc_home)))
    ]
    for load in loads:
        load.start()

    bands = (a + n_lat - 1) // n_lat + (2 * n_lat - 2 - a) // n_lat
    barrier = pltpu.get_barrier_semaphore()
    across_out = around(b, 2 * lax.rem(b, 2) - 1)
    across_home = around(home, 2 * core - 1)
    doubled = across_out < 2 * (chips // 2)
    for lat_step in (-1, 1, 0):
        def greet(lat_step=lat_step):
            def signal(sector):
                pl.semaphore_signal(
                    barrier, inc=1, device_id=(a + lat_step, sector), device_id_type=MESH
                )
            signal(across_out)
            pl.when(doubled)(lambda: signal(worker(across_out)))
            pl.when(traded)(lambda: signal(worker(across_home)))
            signal(partner)
            if lat_step != 0:
                signal(home)
        if_there(lat_step, greet)

    kept = [p_home, sc_home, ec_home, v_home, se_home, inv_home, coupling_home, ce_home, weight_home, sound_home]
    held = [p_row, sc, ec, v_row, se, inv_dual, coupling, ce, weight, sound]
    given = [p_hbm, sc_hbm, ec_hbm, v_hbm, se_hbm, inv_hbm, coupling_hbm, ce_hbm, weight_hbm, sound_hbm]
    loads += [
        pltpu.make_async_copy(x, y, in_sem.at[k + 2]) for k, (x, y) in enumerate(zip(given[2:], kept[2:]))
    ]
    fills = [pltpu.make_async_copy(x, y, work_sem.at[k]) for k, (x, y) in enumerate(zip(given, held))]
    gifts = [
        pltpu.make_async_remote_copy(
            src_ref=x, dst_ref=y, send_sem=in_sem.at[k], recv_sem=work_sem.at[k],
            device_id=(a, partner), device_id_type=MESH,
        )
        for k, (x, y) in enumerate(zip(kept, held))
    ]
    returns = [
        pltpu.make_async_remote_copy(
            src_ref=x, dst_ref=y, send_sem=in_sem.at[k], recv_sem=work_sem.at[k],
            device_id=(a, partner), device_id_type=MESH,
        )
        for k, (x, y) in enumerate(((pf, pf_home), (vf, vf_home)))
    ]
    for load in loads[2:]:
        load.start()

    @pl.when(jnp.logical_not(traded))
    def _():
        for fill in fills:
            fill.start()

    def clear(p):
        def fill():
            for slot, offset in enumerate(OFFSETS):
                if offset[0] == p:
                    for turn in range(2):
                        p_halo[turn, slot] = jnp.zeros(p_halo.shape[2:], F32)
                    for turn in range(NSUB):
                        v_halo[turn, slot] = jnp.zeros(v_halo.shape[2:], F32)
        return fill

    pl.when(a == 0)(clear(-1))
    pl.when(a == n_lat - 1)(clear(1))
    pf[nlev - nlev % 8 :, :] = jnp.zeros_like(pf[nlev - nlev % 8 :, :])
    work[nlev - nlev % 8 :, :] = jnp.zeros_like(pf[nlev - nlev % 8 :, :])
    vf[...] = jnp.zeros_like(vf)

    def copy(i, route, send, land, ss, rs, turn):
        offsets, sector, place = route
        p, q = offsets[i]
        member = member_of(p, q)
        return pltpu.make_async_remote_copy(
            src_ref=send.at[pl.ds(i * rows, nlev)], dst_ref=land.at[turn, 7 - member, pl.ds(0, nlev)],
            send_sem=ss.at[0], recv_sem=rs.at[0],
            device_id=(a + p, place(around(sector, q))), device_id_type=MESH,
        )

    out_route = (home_sends, home, worker)
    mid_route = (sends, b, worker)
    back_route = (sends, b, lambda sector: sector)
    local = pieces - 1

    def stays(i, route, fn):
        if i == local and route is not mid_route:
            pl.when(jnp.logical_not(traded))(fn)
        else:
            if_there(sends[i][0], fn)

    def launch(batch, route, refs, turn):
        for i in batch:
            stays(i, route, lambda: copy(i, route, *refs, turn).start())
            if i == local and route is not mid_route:
                send, land = refs[:2]
                slot = 7 - member_of(*route[0][i])

                @pl.when(traded)
                def _():
                    land[turn, slot] = send[span(i), :]

    def settle(route, refs, fn):
        send, _, ss, rs = refs
        numbers = {2 + 3 * n for n in ((1, 2) if n_lat > 2 else (n_lat - 1,))}
        total = 2 + 3 * bands
        if route is not mid_route:
            numbers |= {n - 1 for n in numbers}
            total = total - traded.astype(jnp.int32)
        for n in sorted(numbers):
            whole = send.at[pl.ds(0, n * nlev)]
            both = pltpu.make_async_remote_copy(
                src_ref=whole, dst_ref=whole, send_sem=ss.at[0], recv_sem=rs.at[0],
                device_id=(a, partner), device_id_type=MESH,
            )
            pl.when(total == n)(lambda: fn(both))

    def arrive(route, refs):
        settle(route, refs, lambda copies: copies.wait_recv())

    def retire(route, refs):
        settle(route, refs, lambda copies: copies.wait_send())

    def pick(tiles, firsts, index):
        shape = tiles[0].shape
        lane = jnp.broadcast_to(index & (LANES - 1), shape)
        tile = jnp.broadcast_to(index >> 7, shape)
        out = jnp.zeros(shape, tiles[0].dtype)
        for values, first in zip(tiles, firsts):
            moved = jnp.take_along_axis(values, lane, axis=1, mode="promise_in_bounds")
            out = jnp.where(tile == first, moved, out)
        return out

    def own_part(tiles):
        return tiles, range(len(tiles))

    def halo_part(land, turn, group, own):
        slots = [member_of(p, q) for p, q in group]
        return [land[turn, slot] for slot in slots], [own + slot for slot in slots]

    def edge_columns(ref, row, k):
        stop = min(edges, (k + 1) * LANES)
        part = row(ref)[:, k * LANES : stop]
        short = (k + 1) * LANES - stop
        return jnp.pad(part, ((0, 0), (0, short))) if short else part

    def span(i):
        return slice(i * rows, (i + 1) * rows)

    def listed(row_tiles, index):
        shape = (pieces, LANES)
        tiles = [jnp.broadcast_to(tile, shape) for tile in row_tiles]
        return pick(tiles, range(len(tiles)), index)

    def piece_change(i, part):
        low, high = (pick(*part, ec_list[r, i : i + 1, :]) for r in (0, 1))
        return high - low

    def piece_sum(i, part):
        total = None
        for j in range(3):
            term = pick(*part, ce_list[j, i : i + 1, :]) * weight_list[j, i : i + 1, :]
            total = term if total is None else total + term
        return total

    def add_gradient(part, fresh, last):
        for k in range(ecols // LANES):
            cols = slice(k * LANES, (k + 1) * LANES)
            taken = [
                pick(*part, spread(edge_columns(ec, lambda ref: ref[0, r : r + 1, :], k), cells, ccols))
                for r in (0, 1)
            ]
            change = taken[1] - taken[0]
            total = change if fresh else grad[:, cols] + change
            if last:
                scale = step_scale * edge_columns(inv_dual, lambda ref: ref[...], k)
                vf[:, cols] = vf[:, cols] - scale * total
            else:
                grad[:, cols] = total

    def add_divergence(part, fresh, last, sides, factors, speeds, values):
        for k in range(ccols // LANES):
            cols = slice(k * LANES, (k + 1) * LANES)
            total = None if fresh else div[:, cols]
            for j in range(3):
                term = pick(*part, spread(sides[j, :, cols], edges, ecols)) * factors[j, :, cols]
                total = term if total is None else total + term
            if last:
                right = values[:, cols] - speeds[:, cols] * total
                work[0:nlev, cols] = right[0:nlev] * t_inv[:, cols]
            else:
                div[:, cols] = total

    def eliminate(couple, put):
        ups = {}
        for k in [*range(middle), *range(nlev - 1, middle - 1, -1)]:
            here, below_it = couple(k), couple(k - 1) if k else None
            diagonal = 1.0 + here if k == 0 else 1.0 + below_it + here
            toward, away = (here, below_it) if k < middle else (below_it, here)
            last = ups.get(k - 1 if k < middle else k + 1)
            inverse = 1.0 / (diagonal if last is None else diagonal - away * last)
            ups[k] = toward * inverse
            put(k, inverse, None if last is None else away * inverse, ups[k])
        return 1.0 / (1.0 - ups[middle - 1] * ups[middle])

    def sweep(scaled, low, up, mid, hold, held, put):
        top = bottom = None
        for step in range(max(middle, nlev - middle)):
            k = step
            if k < middle:
                top = scaled(k) if top is None else scaled(k) + low(k) * top
                hold(k, top)
            k = nlev - 1 - step
            if k >= middle:
                bottom = scaled(k) if bottom is None else scaled(k) + low(k) * bottom
                hold(k, bottom)
        bottom = (bottom + up(middle) * top) * mid
        top = top + up(middle - 1) * bottom
        put(middle, bottom)
        put(middle - 1, top)
        for step in range(1, max(middle, nlev - middle)):
            k = middle - 1 - step
            if k >= 0:
                top = held(k) + up(k) * top
                put(k, top)
            k = middle + step
            if k < nlev:
                bottom = held(k) + up(k) * bottom
                put(k, bottom)

    def level(k):
        return slice(k, k + 1)

    def across(k, batch):
        return pl.ds(k + batch.start * rows, len(batch), stride=rows)

    def own_columns(coupling):
        def put(k, inverse, low, up):
            t_inv[level(k), :] = inverse
            t_up[level(k), :] = up
            if low is not None:
                t_low[level(k), :] = low
        t_mid[...] = eliminate(lambda k: coupling[k], put)

    def piece_columns():
        for k in range(nlev):
            work[level(k), :] = coupling[k]
        tiles = own_part(tiles_of(work, ccols))
        for i in range(pieces):
            s_div[span(i), :] = pick(*tiles, sc_list[i : i + 1, :])

        def put(k, inverse, low, up):
            s_inv[k] = inverse
            s_up[k] = up
            if low is not None:
                s_low[k] = low
        s_mid[...] = eliminate(lambda k: s_div[across(k, range(pieces)), :], put)

    def solve_pieces(batch):
        kept = {}
        some = slice(batch.start, batch.stop)

        def put(k, value):
            p_send[across(k, batch), :] = value
        sweep(
            lambda k: s_div[across(k, batch), :] * s_inv[k, some], lambda k: s_low[k, some],
            lambda k: s_up[k, some], s_mid[some, :], kept.__setitem__, kept.__getitem__, put,
        )

    def solve_own(put):
        def hold(k, value):
            work[level(k), :] = value
        sweep(
            lambda k: work[level(k), :], lambda k: t_low[level(k), :], lambda k: t_up[level(k), :], t_mid[...],
            hold, lambda k: work[level(k), :], put,
        )

    h_refs = (h_send, p_halo, p_ss, p_rs)
    p_refs = (p_send, p_halo, p_ss, p_rs)
    v_refs = (v_send, v_halo, v_ss, v_rs)
    f_refs = (v_send, v_halo, v_ss, f_rs)
    for load in loads[:2]:
        load.wait()
    for k in range(nlev):
        pf[level(k), :] = p_home[k]
    own = own_part(tiles_of(pf, ccols))
    for i, offset in enumerate(home_sends):
        h_send[span(i), :] = pick(*own, sc_home[0, pl.ds(member_of(*offset), 1), :])
    reached = 2 + doubled.astype(jnp.int32) + traded.astype(jnp.int32)
    pl.semaphore_wait(barrier, reached + (reached + 1) * bands)
    launch(range(pieces), out_route, h_refs, 0)
    for load in loads[2:]:
        load.wait()

    @pl.when(traded)
    def _():
        for gift in gifts:
            gift.start()
        for gift in gifts:
            gift.wait_recv()

    @pl.when(jnp.logical_not(traded))
    def _():
        for fill in fills:
            fill.wait()

    for k in range(nlev):
        pf[level(k), :] = p_row[k]
        vf[level(k), 0:edges] = v_row[k]
    for i, offset in enumerate(sends):
        sc_list[i : i + 1, :] = sc[0, pl.ds(member_of(*offset), 1), :]
        se_list[i : i + 1, :] = se[0, pl.ds(member_of(*offset), 1), :]
    own = own_part(tiles_of(pf, ccols))
    for i in range(pieces):
        p_send[span(i), :] = pick(*own, sc_list[i : i + 1, :])
    blocks = range(ecols // LANES)
    index = se_list[...]
    for r in (0, 1):
        row = [edge_columns(ec, lambda ref: ref[0, r : r + 1, :], k) for k in blocks]
        ec_list[r] = spread(listed(row, index), cells, ccols)
    scale_list[...] = step_scale * listed([edge_columns(inv_dual, lambda ref: ref[...], k) for k in blocks], index)
    own = own_part(tiles_of(vf, ecols))
    for i in range(pieces):
        v_send[span(i), :] = pick(*own, se_list[i : i + 1, :])

    def compose_cells():
        index = sc_list[...]
        cuts = [slice(k * LANES, (k + 1) * LANES) for k in range(ccols // LANES)]
        for j in range(3):
            ce_list[j] = spread(listed([ce[j, :, cut] for cut in cuts], index), edges, ecols)
            weight_list[j] = listed([weight[j, :, cut] for cut in cuts], index)
        sound_list[...] = listed([sound[:, cut] for cut in cuts], index)

    here = (ce, weight, sound, pf)
    for substep in range(NSUB):
        final = substep == NSUB - 1
        turn = substep % 2
        route = mid_route if substep else out_route
        own = own_part(tiles_of(pf, ccols))
        for i in range(pieces):
            s_grad[span(i), :] = piece_change(i, own)
        add_gradient(own, True, False)
        if substep == 0:
            compose_cells()
            piece_columns()
            own_columns(coupling)
        else:
            retire(mid_route, v_refs)
        arrive(route, p_refs)
        part = halo_part(p_halo, turn, sends, ccols // LANES)
        for batch in v_batches:
            for i in batch:
                change = s_grad[span(i), :] + piece_change(i, part)
                v_send[span(i), :] = v_send[span(i), :] - scale_list[i : i + 1, :] * change
            if final:
                launch(batch, back_route, f_refs, substep)
            else:
                launch(batch, mid_route, v_refs, substep)
        add_gradient(part, False, True)
        if final:
            pl.when(traded)(returns[1].start)
            pl.when(traded)(lambda: own_columns(coupling_home))
            pl.when(traded)(returns[0].wait_recv)
            pl.when(traded)(returns[1].wait_recv)

            @pl.when(jnp.logical_not(traded))
            def _():
                pf_home[...] = pf[...]
                vf_home[...] = vf[...]

            for k in range(nlev):
                v_out[k] = vf_home[level(k), 0:edges]
            own = own_part(tiles_of(vf_home, ecols))
            here = (ce_home, weight_home, sound_home, pf_home)
        else:
            own = own_part(tiles_of(vf, ecols))
            for i in range(pieces):
                s_div[span(i), :] = piece_sum(i, own)
        add_divergence(own, True, False, *here)
        if substep in (0, NSUB - 1):
            sent = returns if final else gifts
            pl.when(traded)(lambda: [x.wait_send() for x in sent] and None)

        retire(route, h_refs if substep == 0 else p_refs)
        if final:
            arrive(back_route, f_refs)
            part = halo_part(v_halo, substep, home_sends, ecols // LANES)

            def put(k, value):
                p_out[k] = value
        else:
            arrive(mid_route, v_refs)
            part = halo_part(v_halo, substep, sends, ecols // LANES)
            for batch in p_batches:
                for i in batch:
                    total = s_div[span(i), :] + piece_sum(i, part)
                    s_div[span(i), :] = p_send[span(i), :] - sound_list[i : i + 1, :] * total
                solve_pieces(batch)
                launch(batch, mid_route, p_refs, 1 - turn)

            def put(k, value):
                pf[level(k), :] = value
        add_divergence(part, False, True, *here)
        solve_own(put)
        if substep == NSUB - 2:
            pl.when(traded)(returns[0].start)

    retire(back_route, f_refs)


def write_out(p_ref, v_ref, p_out, v_out, sem):
    stores = [
        pltpu.make_async_copy(x, y, sem.at[k])
        for k, (x, y) in enumerate(((v_ref, v_out), (p_ref, p_out)))
    ]
    for store in stores:
        store.start()
    for store in stores:
        store.wait()


def level_major(x):
    return jnp.transpose(x, (1, 0, 2))


def on_device(*args):
    pressure, velocity, send_cells = args[0], args[1], args[4]
    n_lat, n_lon = lax.axis_size("lat"), lax.axis_size("lon")
    nlev, cells, edges = pressure.shape[1], pressure.shape[2], velocity.shape[2]
    halo = send_cells.shape[2]
    rows, ecols = round_up(nlev, 32), round_up(edges, 128)
    hbm = pl.BlockSpec(memory_space=pltpu.HBM)
    vmem = pl.BlockSpec(memory_space=pltpu.VMEM)
    args = [level_major(x) if k in (0, 1, 3, 7, 9) else x for k, x in enumerate(args)]

    def body(*refs):
        kernel(n_lat, n_lon, nlev, cells, edges, halo, *refs)

    halo_shape = pltpu.VMEM((2, 8, rows, halo), F32)
    piece_shape = pltpu.VMEM((8 * rows, halo), F32)
    list_shape = pltpu.VMEM((8, halo), F32)
    places = pltpu.VMEM((8, halo), jnp.int32)
    cell_shape = pltpu.VMEM((rows, cells), F32)
    edge_shape = pltpu.VMEM((rows, ecols), F32)
    level_shape = pltpu.VMEM((nlev, cells), F32)
    stack_shape = pltpu.VMEM((nlev, 8, halo), F32)
    outs = pl.pallas_call(
        body,
        name="substeps",
        out_shape=(
            pltpu.VMEM(args[0].shape, F32),
            pltpu.VMEM(args[1].shape, F32),
        ),
        in_specs=[hbm] * len(args),
        out_specs=(vmem, vmem),
        scratch_shapes=[pltpu.VMEM(x.shape, x.dtype) for x in args] * 2 + [
            cell_shape, edge_shape, cell_shape, edge_shape, piece_shape, piece_shape, piece_shape,
            halo_shape, pltpu.VMEM((NSUB, 8, rows, halo), F32),
            level_shape, level_shape, level_shape, pltpu.VMEM((1, cells), F32), cell_shape, edge_shape, cell_shape,
            places, places, pltpu.VMEM((2, 8, halo), jnp.int32), pltpu.VMEM((3, 8, halo), jnp.int32),
            list_shape, pltpu.VMEM((3, 8, halo), F32), list_shape,
            stack_shape, stack_shape, stack_shape, list_shape, piece_shape, piece_shape,
            *[pltpu.SemaphoreType.DMA((1,))] * 5,
            *[pltpu.SemaphoreType.DMA((len(args),))] * 2,
        ],
        compiler_params=pltpu.CompilerParams(
            collective_id=0, has_side_effects=True, vmem_limit_bytes=66_000_000
        ),
    )(*args)
    outs = pl.pallas_call(
        write_out,
        name="write_out",
        out_shape=tuple(jax.ShapeDtypeStruct(x.shape, F32) for x in outs),
        in_specs=[vmem] * 2,
        out_specs=(hbm, hbm),
        scratch_shapes=[pltpu.SemaphoreType.DMA((2,))],
        compiler_params=pltpu.CompilerParams(vmem_limit_bytes=1024 * 1024),
    )(*outs)
    return tuple(level_major(x) for x in outs)


def solution(mesh):
    band = P("lat", None, "lon")
    flat = P("lat", "lon")
    return jax.shard_map(
        on_device,
        mesh=mesh,
        in_specs=(band, band, band, band, band, band, flat, band, flat, band),
        out_specs=(band, band),
        check_vma=False,
    )
```

```python
import math

import jax
import jax.numpy as jnp
from jax import lax
from jax.experimental import pallas as pl
from jax.experimental.pallas import tpu as pltpu
from jax.sharding import PartitionSpec as P

NSUB = 3
OFFSETS = ((-1, -1), (-1, 0), (-1, 1), (0, -1), (0, 1), (1, -1), (1, 0), (1, 1))
LANES = 128
step_scale = 0.5
MESH = pl.DeviceIdType.MESH
F32 = jnp.float32


def round_up(n, m):
    return (n + m - 1) // m * m


def tiles_of(ref, width):
    return [ref[:, k * LANES : (k + 1) * LANES] for k in range(width // LANES)]


def spread(index, own, padded):
    return jnp.where(index >= own, index + (padded - own), index)


def member_of(p, q):
    if isinstance(p, int) and p == 0:
        return 3 + (q + 1) // 2
    return (7 + 5 * p) // 2 + q


def kernel(
    n_lat, n_lon, nlev, cells, edges, halo,
    p_hbm, v_hbm, ec_hbm, ce_hbm, sc_hbm, se_hbm, inv_hbm, weight_hbm, sound_hbm, coupling_hbm,
    p_out, v_out,
    p_home, v_home, ec_home, ce_home, sc_home, se_home, inv_home, weight_home, sound_home, coupling_home,
    p_row, v_row, ec, ce, sc, se, inv_dual, weight, sound, coupling,
    pf, vf, pf_home, vf_home, h_send, p_send, v_send, p_halo, v_halo,
    t_inv, t_low, t_up, t_mid, work, grad, div,
    sc_list, se_list, ec_list, ce_list, scale_list, weight_list, sound_list,
    s_inv, s_low, s_up, s_mid, s_grad, s_div,
    p_ss, p_rs, v_ss, v_rs, f_rs, in_sem, work_sem,
):
    a, home = lax.axis_index("lat"), lax.axis_index("lon")
    chips = n_lon // 2
    chip, core = home // 2, lax.rem(home, 2)
    partner = home + 1 - 2 * core
    traded = chip < chips // 2
    b = jnp.where(traded, partner, home)
    ccols, ecols = pf.shape[1], vf.shape[1]
    rows = pf.shape[0]
    pieces = len(OFFSETS)
    middle = nlev // 2
    side = math.isqrt(n_lat)
    slow = jnp.where(lax.rem(a, side) == side - 1, 1, -1)
    quick = -slow

    def ordered(far):
        near = -far
        return [
            (slow, far), (slow, near), (slow, 0), (quick, far), (0, far),
            (quick, near), (quick, 0), (0, near),
        ]

    home_sends = ordered(2 * core - 1)
    sends = ordered(2 * lax.rem(b, 2) - 1)
    p_batches = (range(0, 2), range(2, 4), range(4, 6), range(6, 8),)
    v_batches = (range(0, 1), range(1, 2), range(2, 4), range(4, 6), range(6, 8),)

    def if_there(p, fn):
        if isinstance(p, int) and p == 0:
            fn()
        else:
            pl.when((a + p >= 0) & (a + p < n_lat))(fn)

    def around(sector, q):
        return lax.rem(sector + q + n_lon, n_lon)

    def worker(sector):
        return jnp.where(sector < 2 * (chips // 2), sector + 1 - 2 * lax.rem(sector, 2), sector)

    loads = [
        pltpu.make_async_copy(x, y, in_sem.at[k])
        for k, (x, y) in enumerate(((p_hbm, p_home), (sc_hbm, sc_home)))
    ]
    for load in loads:
        load.start()

    bands = (a + n_lat - 1) // n_lat + (2 * n_lat - 2 - a) // n_lat
    barrier = pltpu.get_barrier_semaphore()
    across_out = around(b, 2 * lax.rem(b, 2) - 1)
    across_home = around(home, 2 * core - 1)
    doubled = across_out < 2 * (chips // 2)
    for lat_step in (-1, 1, 0):
        def greet(lat_step=lat_step):
            def signal(sector):
                pl.semaphore_signal(
                    barrier, inc=1, device_id=(a + lat_step, sector), device_id_type=MESH
                )
            signal(across_out)
            pl.when(doubled)(lambda: signal(worker(across_out)))
            pl.when(traded)(lambda: signal(worker(across_home)))
            signal(partner)
            if lat_step != 0:
                signal(home)
        if_there(lat_step, greet)

    kept = [p_home, sc_home, ec_home, v_home, se_home, inv_home, coupling_home, ce_home, weight_home, sound_home]
    held = [p_row, sc, ec, v_row, se, inv_dual, coupling, ce, weight, sound]
    given = [p_hbm, sc_hbm, ec_hbm, v_hbm, se_hbm, inv_hbm, coupling_hbm, ce_hbm, weight_hbm, sound_hbm]
    loads += [
        pltpu.make_async_copy(x, y, in_sem.at[k + 2]) for k, (x, y) in enumerate(zip(given[2:], kept[2:]))
    ]
    fills = [pltpu.make_async_copy(x, y, work_sem.at[k]) for k, (x, y) in enumerate(zip(given, held))]
    gifts = [
        pltpu.make_async_remote_copy(
            src_ref=x, dst_ref=y, send_sem=in_sem.at[k], recv_sem=work_sem.at[k],
            device_id=(a, partner), device_id_type=MESH,
        )
        for k, (x, y) in enumerate(zip(kept, held))
    ]
    returns = [
        pltpu.make_async_remote_copy(
            src_ref=x, dst_ref=y, send_sem=in_sem.at[k], recv_sem=work_sem.at[k],
            device_id=(a, partner), device_id_type=MESH,
        )
        for k, (x, y) in enumerate(((pf, pf_home), (vf, vf_home)))
    ]
    for load in loads[2:]:
        load.start()

    @pl.when(jnp.logical_not(traded))
    def _():
        for fill in fills:
            fill.start()

    def clear(p):
        def fill():
            for slot, offset in enumerate(OFFSETS):
                if offset[0] == p:
                    for turn in range(2):
                        p_halo[turn, slot] = jnp.zeros(p_halo.shape[2:], F32)
                    for turn in range(NSUB):
                        v_halo[turn, slot] = jnp.zeros(v_halo.shape[2:], F32)
        return fill

    pl.when(a == 0)(clear(-1))
    pl.when(a == n_lat - 1)(clear(1))
    pf[nlev - nlev % 8 :, :] = jnp.zeros_like(pf[nlev - nlev % 8 :, :])
    work[nlev - nlev % 8 :, :] = jnp.zeros_like(pf[nlev - nlev % 8 :, :])
    vf[...] = jnp.zeros_like(vf)

    def copy(i, route, send, land, ss, rs, turn):
        offsets, sector, place = route
        p, q = offsets[i]
        member = member_of(p, q)
        return pltpu.make_async_remote_copy(
            src_ref=send.at[pl.ds(i * rows, nlev)], dst_ref=land.at[turn, 7 - member, pl.ds(0, nlev)],
            send_sem=ss.at[0], recv_sem=rs.at[0],
            device_id=(a + p, place(around(sector, q))), device_id_type=MESH,
        )

    out_route = (home_sends, home, worker)
    mid_route = (sends, b, worker)
    back_route = (sends, b, lambda sector: sector)
    local = pieces - 1

    def stays(i, route, fn):
        if i == local and route is not mid_route:
            pl.when(jnp.logical_not(traded))(fn)
        else:
            if_there(sends[i][0], fn)

    def launch(batch, route, refs, turn):
        for i in batch:
            stays(i, route, lambda: copy(i, route, *refs, turn).start())
            if i == local and route is not mid_route:
                send, land = refs[:2]
                slot = 7 - member_of(*route[0][i])

                @pl.when(traded)
                def _():
                    land[turn, slot] = send[span(i), :]

    def settle(route, refs, fn):
        send, _, ss, rs = refs
        numbers = {2 + 3 * n for n in ((1, 2) if n_lat > 2 else (n_lat - 1,))}
        total = 2 + 3 * bands
        if route is not mid_route:
            numbers |= {n - 1 for n in numbers}
            total = total - traded.astype(jnp.int32)
        for n in sorted(numbers):
            whole = send.at[pl.ds(0, n * nlev)]
            both = pltpu.make_async_remote_copy(
                src_ref=whole, dst_ref=whole, send_sem=ss.at[0], recv_sem=rs.at[0],
                device_id=(a, partner), device_id_type=MESH,
            )
            pl.when(total == n)(lambda: fn(both))

    def arrive(route, refs):
        settle(route, refs, lambda copies: copies.wait_recv())

    def retire(route, refs):
        settle(route, refs, lambda copies: copies.wait_send())

    def pick(tiles, firsts, index):
        shape = tiles[0].shape
        lane = jnp.broadcast_to(index & (LANES - 1), shape)
        tile = jnp.broadcast_to(index >> 7, shape)
        out = jnp.zeros(shape, tiles[0].dtype)
        for values, first in zip(tiles, firsts):
            moved = jnp.take_along_axis(values, lane, axis=1, mode="promise_in_bounds")
            out = jnp.where(tile == first, moved, out)
        return out

    def own_part(tiles):
        return tiles, range(len(tiles))

    def halo_part(land, turn, group, own):
        slots = [member_of(p, q) for p, q in group]
        return [land[turn, slot] for slot in slots], [own + slot for slot in slots]

    def edge_columns(ref, row, k):
        stop = min(edges, (k + 1) * LANES)
        part = row(ref)[:, k * LANES : stop]
        short = (k + 1) * LANES - stop
        return jnp.pad(part, ((0, 0), (0, short))) if short else part

    def span(i):
        return slice(i * rows, (i + 1) * rows)

    def listed(row_tiles, index):
        shape = (pieces, LANES)
        tiles = [jnp.broadcast_to(tile, shape) for tile in row_tiles]
        return pick(tiles, range(len(tiles)), index)

    def piece_change(i, part):
        low, high = (pick(*part, ec_list[r, i : i + 1, :]) for r in (0, 1))
        return high - low

    def piece_sum(i, part):
        total = None
        for j in range(3):
            term = pick(*part, ce_list[j, i : i + 1, :]) * weight_list[j, i : i + 1, :]
            total = term if total is None else total + term
        return total

    def add_gradient(part, fresh, last):
        for k in range(ecols // LANES):
            cols = slice(k * LANES, (k + 1) * LANES)
            taken = [
                pick(*part, spread(edge_columns(ec, lambda ref: ref[0, r : r + 1, :], k), cells, ccols))
                for r in (0, 1)
            ]
            change = taken[1] - taken[0]
            total = change if fresh else grad[:, cols] + change
            if last:
                scale = step_scale * edge_columns(inv_dual, lambda ref: ref[...], k)
                vf[:, cols] = vf[:, cols] - scale * total
            else:
                grad[:, cols] = total

    def add_divergence(part, fresh, last, sides, factors, speeds, values):
        for k in range(ccols // LANES):
            cols = slice(k * LANES, (k + 1) * LANES)
            total = None if fresh else div[:, cols]
            for j in range(3):
                term = pick(*part, spread(sides[j, :, cols], edges, ecols)) * factors[j, :, cols]
                total = term if total is None else total + term
            if last:
                right = values[:, cols] - speeds[:, cols] * total
                work[0:nlev, cols] = right[0:nlev] * t_inv[:, cols]
            else:
                div[:, cols] = total

    def eliminate(couple, put):
        ups = {}
        for k in [*range(middle), *range(nlev - 1, middle - 1, -1)]:
            here, below_it = couple(k), couple(k - 1) if k else None
            diagonal = 1.0 + here if k == 0 else 1.0 + below_it + here
            toward, away = (here, below_it) if k < middle else (below_it, here)
            last = ups.get(k - 1 if k < middle else k + 1)
            inverse = 1.0 / (diagonal if last is None else diagonal - away * last)
            ups[k] = toward * inverse
            put(k, inverse, None if last is None else away * inverse, ups[k])
        return 1.0 / (1.0 - ups[middle - 1] * ups[middle])

    def sweep(scaled, low, up, mid, hold, held, put):
        top = bottom = None
        for step in range(max(middle, nlev - middle)):
            k = step
            if k < middle:
                top = scaled(k) if top is None else scaled(k) + low(k) * top
                hold(k, top)
            k = nlev - 1 - step
            if k >= middle:
                bottom = scaled(k) if bottom is None else scaled(k) + low(k) * bottom
                hold(k, bottom)
        bottom = (bottom + up(middle) * top) * mid
        top = top + up(middle - 1) * bottom
        put(middle, bottom)
        put(middle - 1, top)
        for step in range(1, max(middle, nlev - middle)):
            k = middle - 1 - step
            if k >= 0:
                top = held(k) + up(k) * top
                put(k, top)
            k = middle + step
            if k < nlev:
                bottom = held(k) + up(k) * bottom
                put(k, bottom)

    def level(k):
        return slice(k, k + 1)

    def across(k, batch):
        return pl.ds(k + batch.start * rows, len(batch), stride=rows)

    def own_columns(coupling):
        def put(k, inverse, low, up):
            t_inv[level(k), :] = inverse
            t_up[level(k), :] = up
            if low is not None:
                t_low[level(k), :] = low
        t_mid[...] = eliminate(lambda k: coupling[k], put)

    def piece_columns():
        for k in range(nlev):
            work[level(k), :] = coupling[k]
        tiles = own_part(tiles_of(work, ccols))
        for i in range(pieces):
            s_div[span(i), :] = pick(*tiles, sc_list[i : i + 1, :])

        def put(k, inverse, low, up):
            s_inv[k] = inverse
            s_up[k] = up
            if low is not None:
                s_low[k] = low
        s_mid[...] = eliminate(lambda k: s_div[across(k, range(pieces)), :], put)

    def solve_pieces(batch):
        kept = {}
        some = slice(batch.start, batch.stop)

        def put(k, value):
            p_send[across(k, batch), :] = value
        sweep(
            lambda k: s_div[across(k, batch), :] * s_inv[k, some], lambda k: s_low[k, some],
            lambda k: s_up[k, some], s_mid[some, :], kept.__setitem__, kept.__getitem__, put,
        )

    def solve_own(put):
        def hold(k, value):
            work[level(k), :] = value
        sweep(
            lambda k: work[level(k), :], lambda k: t_low[level(k), :], lambda k: t_up[level(k), :], t_mid[...],
            hold, lambda k: work[level(k), :], put,
        )

    h_refs = (h_send, p_halo, p_ss, p_rs)
    p_refs = (p_send, p_halo, p_ss, p_rs)
    v_refs = (v_send, v_halo, v_ss, v_rs)
    f_refs = (v_send, v_halo, v_ss, f_rs)
    for load in loads[:2]:
        load.wait()
    for k in range(nlev):
        pf[level(k), :] = p_home[k]
    own = own_part(tiles_of(pf, ccols))
    for i, offset in enumerate(home_sends):
        h_send[span(i), :] = pick(*own, sc_home[0, pl.ds(member_of(*offset), 1), :])
    reached = 2 + doubled.astype(jnp.int32) + traded.astype(jnp.int32)
    pl.semaphore_wait(barrier, reached + (reached + 1) * bands)
    launch(range(pieces), out_route, h_refs, 0)
    for load in loads[2:]:
        load.wait()

    @pl.when(traded)
    def _():
        for gift in gifts:
            gift.start()
        for gift in gifts:
            gift.wait_recv()

    @pl.when(jnp.logical_not(traded))
    def _():
        for fill in fills:
            fill.wait()

    for k in range(nlev):
        pf[level(k), :] = p_row[k]
        vf[level(k), 0:edges] = v_row[k]
    for i, offset in enumerate(sends):
        sc_list[i : i + 1, :] = sc[0, pl.ds(member_of(*offset), 1), :]
        se_list[i : i + 1, :] = se[0, pl.ds(member_of(*offset), 1), :]
    own = own_part(tiles_of(pf, ccols))
    for i in range(pieces):
        p_send[span(i), :] = pick(*own, sc_list[i : i + 1, :])
    blocks = range(ecols // LANES)
    index = se_list[...]
    for r in (0, 1):
        row = [edge_columns(ec, lambda ref: ref[0, r : r + 1, :], k) for k in blocks]
        ec_list[r] = spread(listed(row, index), cells, ccols)
    scale_list[...] = step_scale * listed([edge_columns(inv_dual, lambda ref: ref[...], k) for k in blocks], index)
    own = own_part(tiles_of(vf, ecols))
    for i in range(pieces):
        v_send[span(i), :] = pick(*own, se_list[i : i + 1, :])

    def compose_cells():
        index = sc_list[...]
        cuts = [slice(k * LANES, (k + 1) * LANES) for k in range(ccols // LANES)]
        for j in range(3):
            ce_list[j] = spread(listed([ce[j, :, cut] for cut in cuts], index), edges, ecols)
            weight_list[j] = listed([weight[j, :, cut] for cut in cuts], index)
        sound_list[...] = listed([sound[:, cut] for cut in cuts], index)

    here = (ce, weight, sound, pf)
    for substep in range(NSUB):
        final = substep == NSUB - 1
        turn = substep % 2
        route = mid_route if substep else out_route
        own = own_part(tiles_of(pf, ccols))
        for i in range(pieces):
            s_grad[span(i), :] = piece_change(i, own)
        add_gradient(own, True, False)
        if substep == 0:
            compose_cells()
            piece_columns()
            own_columns(coupling)
        else:
            retire(mid_route, v_refs)
        arrive(route, p_refs)
        part = halo_part(p_halo, turn, sends, ccols // LANES)
        for batch in v_batches:
            for i in batch:
                change = s_grad[span(i), :] + piece_change(i, part)
                v_send[span(i), :] = v_send[span(i), :] - scale_list[i : i + 1, :] * change
            if final:
                launch(batch, back_route, f_refs, substep)
            else:
                launch(batch, mid_route, v_refs, substep)
        add_gradient(part, False, True)
        if final:
            pl.when(traded)(returns[1].start)
            pl.when(traded)(lambda: own_columns(coupling_home))
            pl.when(traded)(returns[0].wait_recv)
            pl.when(traded)(returns[1].wait_recv)

            @pl.when(jnp.logical_not(traded))
            def _():
                pf_home[...] = pf[...]
                vf_home[...] = vf[...]

            for k in range(nlev):
                v_out[k] = vf_home[level(k), 0:edges]
            own = own_part(tiles_of(vf_home, ecols))
            here = (ce_home, weight_home, sound_home, pf_home)
        else:
            own = own_part(tiles_of(vf, ecols))
            for i in range(pieces):
                s_div[span(i), :] = piece_sum(i, own)
        add_divergence(own, True, False, *here)
        if substep in (0, NSUB - 1):
            sent = returns if final else gifts
            pl.when(traded)(lambda: [x.wait_send() for x in sent] and None)

        retire(route, h_refs if substep == 0 else p_refs)
        if final:
            arrive(back_route, f_refs)
            part = halo_part(v_halo, substep, home_sends, ecols // LANES)

            def put(k, value):
                p_out[k] = value
        else:
            arrive(mid_route, v_refs)
            part = halo_part(v_halo, substep, sends, ecols // LANES)
            for batch in p_batches:
                for i in batch:
                    total = s_div[span(i), :] + piece_sum(i, part)
                    s_div[span(i), :] = p_send[span(i), :] - sound_list[i : i + 1, :] * total
                solve_pieces(batch)
                launch(batch, mid_route, p_refs, 1 - turn)

            def put(k, value):
                pf[level(k), :] = value
        add_divergence(part, False, True, *here)
        solve_own(put)
        if substep == NSUB - 2:
            pl.when(traded)(returns[0].start)

    retire(back_route, f_refs)


def write_out(p_ref, v_ref, p_out, v_out, sem):
    stores = [
        pltpu.make_async_copy(x, y, sem.at[k])
        for k, (x, y) in enumerate(((v_ref, v_out), (p_ref, p_out)))
    ]
    for store in stores:
        store.start()
    for store in stores:
        store.wait()


def level_major(x):
    return jnp.transpose(x, (1, 0, 2))


def on_device(*args):
    pressure, velocity, send_cells = args[0], args[1], args[4]
    n_lat, n_lon = lax.axis_size("lat"), lax.axis_size("lon")
    nlev, cells, edges = pressure.shape[1], pressure.shape[2], velocity.shape[2]
    halo = send_cells.shape[2]
    rows, ecols = round_up(nlev, 32), round_up(edges, 128)
    hbm = pl.BlockSpec(memory_space=pltpu.HBM)
    vmem = pl.BlockSpec(memory_space=pltpu.VMEM)
    args = [level_major(x) if k in (0, 1, 3, 7, 9) else x for k, x in enumerate(args)]

    def body(*refs):
        kernel(n_lat, n_lon, nlev, cells, edges, halo, *refs)

    halo_shape = pltpu.VMEM((2, 8, rows, halo), F32)
    piece_shape = pltpu.VMEM((8 * rows, halo), F32)
    list_shape = pltpu.VMEM((8, halo), F32)
    places = pltpu.VMEM((8, halo), jnp.int32)
    cell_shape = pltpu.VMEM((rows, cells), F32)
    edge_shape = pltpu.VMEM((rows, ecols), F32)
    level_shape = pltpu.VMEM((nlev, cells), F32)
    stack_shape = pltpu.VMEM((nlev, 8, halo), F32)
    outs = pl.pallas_call(
        body,
        name="substeps",
        out_shape=(
            pltpu.VMEM(args[0].shape, F32),
            pltpu.VMEM(args[1].shape, F32),
        ),
        in_specs=[hbm] * len(args),
        out_specs=(vmem, vmem),
        scratch_shapes=[pltpu.VMEM(x.shape, x.dtype) for x in args] * 2 + [
            cell_shape, edge_shape, cell_shape, edge_shape, piece_shape, piece_shape, piece_shape,
            halo_shape, pltpu.VMEM((NSUB, 8, rows, halo), F32),
            level_shape, level_shape, level_shape, pltpu.VMEM((1, cells), F32), cell_shape, edge_shape, cell_shape,
            places, places, pltpu.VMEM((2, 8, halo), jnp.int32), pltpu.VMEM((3, 8, halo), jnp.int32),
            list_shape, pltpu.VMEM((3, 8, halo), F32), list_shape,
            stack_shape, stack_shape, stack_shape, list_shape, piece_shape, piece_shape,
            *[pltpu.SemaphoreType.DMA((1,))] * 5,
            *[pltpu.SemaphoreType.DMA((len(args),))] * 2,
        ],
        compiler_params=pltpu.CompilerParams(
            collective_id=0, has_side_effects=True, vmem_limit_bytes=66_000_000
        ),
    )(*args)
    outs = pl.pallas_call(
        write_out,
        name="write_out",
        out_shape=tuple(jax.ShapeDtypeStruct(x.shape, F32) for x in outs),
        in_specs=[vmem] * 2,
        out_specs=(hbm, hbm),
        scratch_shapes=[pltpu.SemaphoreType.DMA((2,))],
        compiler_params=pltpu.CompilerParams(vmem_limit_bytes=1024 * 1024),
    )(*outs)
    return tuple(level_major(x) for x in outs)


def solution(mesh):
    band = P("lat", None, "lon")
    flat = P("lat", "lon")
    return jax.shard_map(
        on_device,
        mesh=mesh,
        in_specs=(band, band, band, band, band, band, flat, band, flat, band),
        out_specs=(band, band),
        check_vma=False,
    )
```
